32 devices in a mesh: lon: 8 (over y, x, core), lat: 4 (over z).
Axes of the slice: x: 2, y: 2, z: 4, core: 2. Of those that a mesh axis runs over, the one named last changes fastest.
Arguments:
- surface_forcing: float32 [96, 1024], P('lat', 'lon'), may hold values from -33 to 33
- sea_mask: int32 [96, 1024], P('lat', 'lon'), may hold values 0 or 1
- level_count: int32 [96, 1024], P('lat', 'lon'), may hold values from 1 to 40
- state: float32 [4, 40, 96, 1024], P(None, None, 'lat', 'lon'), may hold values from -6 to 6
Outputs:
- surface_height: float32 [96, 1024], P('lat', 'lon')
- residual: float32 [96, 1024], P('lat', 'lon')
- tendency: float32 [4, 40, 96, 1024], P(None, None, 'lat', 'lon')
The draws below stay inside these ranges and needn't reach their ends.
All inputs are finite; a program needn't handle non-finite values. No bound on the sum of `sea_mask` on one device may be relied on, other than what follows from the above.
Results may differ from the reference program's by a relative error of at most 0.0003.
Values sent between devices are 32-bit elements; how exact they have to be, the bound alone decides.
A program may use at most 64 MiB of HBM per device.

```python
import jax
import jax.numpy as jnp
from jax import lax

LEV = 40
ITERS = 4
NX = 1024
NY = 96


def draw_surface_forcing(key, part):
    row_frac = jnp.arange(NY, dtype=jnp.float32) / NY
    column_frac = jnp.arange(NX, dtype=jnp.float32) / NX
    growth = jnp.exp(jnp.log(3.0) * (row_frac[:, None] + column_frac[None, :]))
    key_rough = jax.random.fold_in(jax.random.fold_in(key, 11), 0)
    values = jax.random.truncated_normal(key_rough, -3.0, 3.0, (NY, NX), jnp.float32) * growth
    return values


def plant(values, own_key, least, top_value):
    spot = [jax.random.randint(jax.random.fold_in(own_key, axis), (), 0, length) for axis, length in enumerate(values.shape)]
    main_axis = values.shape.index(max(values.shape))
    neighbour = spot[:main_axis] + [(spot[main_axis] + 1) % values.shape[main_axis]] + spot[main_axis + 1:]
    return values.at[tuple(spot)].set(least).at[tuple(neighbour)].set(top_value)


def shard_levels(key, shape, pieces, low, largest):
    def one(axis_at, parts):
        draws = jax.random.uniform(jax.random.fold_in(jax.random.fold_in(key, 6), axis_at), (parts,), jnp.float32, low / len(pieces), largest / len(pieces))
        return jnp.repeat(jnp.exp(draws), shape[axis_at] // parts).reshape((-1,) + (1,) * (len(shape) - axis_at - 1))

    gain = one(*pieces[0])
    for cut in pieces[1:]:
        gain = gain * one(*cut)
    return gain


def centred(key, dims, scale, most, cuts=(), kind=jnp.bfloat16):
    entries = scale * jax.random.normal(key, dims, jnp.float32)
    if cuts:
        entries = entries * shard_levels(key, dims, cuts, -0.22, 0.18)
    return jnp.clip(entries, -most, most).astype(kind)


def setup_inputs(seed: int = 0) -> dict:
    arg_keys = jax.random.split(jax.random.key(seed), 5)
    return {
        "surface_forcing": draw_surface_forcing(jax.random.fold_in(arg_keys[4], 71), 0),
        "sea_mask": plant((jax.random.randint(arg_keys[1], (NY, NX), 0, 4) < 3).astype(jnp.int32), jax.random.fold_in(arg_keys[1], 1), 0, 1),
        "level_count": plant(jax.random.randint(arg_keys[2], (NY, NX), 1, LEV + 1), jax.random.fold_in(arg_keys[2], 1), 1, LEV).astype(jnp.int32),
        "state": centred(arg_keys[3], (4, LEV, NY, NX), 1.0, 6.0, ((2, 4), (3, 8)), jnp.float32),
    }


damping = 0.05
face_scale = 1.0
viscosity = 0.02


def wrap_pad(field, width):
    field = jnp.concatenate([field[..., -width:], field, field[..., :width]], axis=-1)
    spec = [(0, 0)] * (field.ndim - 2) + [(width, width), (0, 0)]
    return jnp.pad(field, spec)


def trim_rims(field, margin):
    return field[..., margin:field.shape[-2] - margin, margin:field.shape[-1] - margin]


def face_coeffs(depth, width_out, width_in):
    offset = width_in - width_out
    height = depth.shape[0] - 2 * offset
    breadth = depth.shape[1] - 2 * offset
    center = depth[offset:offset + height, offset:offset + breadth]
    east_face = face_scale * jnp.minimum(center, depth[offset:offset + height, offset + 1:offset + 1 + breadth])
    west_face = face_scale * jnp.minimum(center, depth[offset:offset + height, offset - 1:offset - 1 + breadth])
    north_face = face_scale * jnp.minimum(center, depth[offset + 1:offset + 1 + height, offset:offset + breadth])
    south_face = face_scale * jnp.minimum(center, depth[offset - 1:offset - 1 + height, offset:offset + breadth])
    diagonal = damping + east_face + west_face + north_face + south_face
    return diagonal, east_face, west_face, north_face, south_face


def operator_apply(padded, coeffs):
    diagonal, east_face, west_face, north_face, south_face = coeffs
    return (diagonal * padded[1:-1, 1:-1] - east_face * padded[1:-1, 2:] - west_face * padded[1:-1, :-2]
            - north_face * padded[2:, 1:-1] - south_face * padded[:-2, 1:-1])


def laplace(field, active):
    center = field[..., 1:-1, 1:-1]
    active_center = active[..., 1:-1, 1:-1]
    east_part = active_center * active[..., 1:-1, 2:] * (field[..., 1:-1, 2:] - center)
    west_part = active_center * active[..., 1:-1, :-2] * (center - field[..., 1:-1, :-2])
    north_part = active_center * active[..., 2:, 1:-1] * (field[..., 2:, 1:-1] - center)
    south_part = active_center * active[..., :-2, 1:-1] * (center - field[..., :-2, 1:-1])
    return east_part - west_part + north_part - south_part


def advect(field, active):
    east_flow = field[2]
    north_flow = field[3]
    center = field[..., 1:-1, 1:-1]
    active_center = active[..., 1:-1, 1:-1]
    flow_center = east_flow[..., 1:-1, 1:-1]
    lift_center = north_flow[..., 1:-1, 1:-1]
    east_speed = 0.25 * active_center * active[..., 1:-1, 2:] * (flow_center + east_flow[..., 1:-1, 2:])
    west_speed = 0.25 * active_center * active[..., 1:-1, :-2] * (flow_center + east_flow[..., 1:-1, :-2])
    north_speed = 0.25 * active_center * active[..., 2:, 1:-1] * (lift_center + north_flow[..., 2:, 1:-1])
    south_speed = 0.25 * active_center * active[..., :-2, 1:-1] * (lift_center + north_flow[..., :-2, 1:-1])
    return (east_speed * (center + field[..., 1:-1, 2:]) - west_speed * (center + field[..., 1:-1, :-2])
            + north_speed * (center + field[..., 2:, 1:-1]) - south_speed * (center + field[..., :-2, 1:-1]))


def tendency_of(state_wide, active_wide):
    inner_active = trim_rims(active_wide, 1)
    smoothed = laplace(laplace(state_wide, active_wide), inner_active)
    flux = advect(trim_rims(state_wide, 1), inner_active)
    return trim_rims(active_wide, 2) * (-flux - viscosity * smoothed)


def reference(surface_forcing, sea_mask, level_count, state):
    sea = sea_mask.astype(jnp.float32)
    depth = sea * level_count.astype(jnp.float32) / LEV
    coeffs = face_coeffs(wrap_pad(depth, 1), 0, 1)
    forcing = sea * surface_forcing
    solution = jnp.zeros_like(forcing)
    residual = forcing
    search = residual / coeffs[0]
    direction = search
    product = jnp.sum(residual * search)
    for step_index in range(ITERS):
        image = operator_apply(wrap_pad(direction, 1), coeffs)
        alpha_step = product / jnp.sum(direction * image)
        solution = solution + alpha_step * direction
        residual = residual - alpha_step * image
        if step_index + 1 < ITERS:
            search = residual / coeffs[0]
            product_next = jnp.sum(residual * search)
            direction = search + (product_next / product) * direction
            product = product_next

    def level_tendency(level):
        active = (level < level_count).astype(jnp.float32) * sea
        layer = lax.dynamic_index_in_dim(state, level, 1, keepdims=False)
        return tendency_of(wrap_pad(layer, 2), wrap_pad(active, 2))

    stacked = lax.map(level_tendency, jnp.arange(LEV, dtype=jnp.int32))
    return solution, residual, jnp.moveaxis(stacked, 0, 1)
```

```python
import functools

import jax
import jax.numpy as jnp
from jax import lax
from jax.experimental import pallas as pl
from jax.experimental.pallas import tpu as pltpu
from jax.sharding import PartitionSpec as P

ITERS = 4
DAMPING = 0.05
VISCOSITY = 0.02
COLS = 4
MESH = pl.DeviceIdType.MESH


def east(a, b, lane):
    ra, rb = pltpu.roll(a, 127, 1), pltpu.roll(b, 127, 1)
    keep = lane < 127
    return jnp.where(keep, ra, rb), jnp.where(keep, rb, ra)


def west(a, b, lane):
    ra, rb = pltpu.roll(a, 1, 1), pltpu.roll(b, 1, 1)
    keep = lane > 0
    return jnp.where(keep, ra, rb), jnp.where(keep, rb, ra)


def north(x):
    return pltpu.roll(x, x.shape[0] - 1, 0)


def south(x):
    return pltpu.roll(x, 1, 0)


def lanes(x):
    return lax.broadcasted_iota(jnp.int32, x.shape, 1)


def kernel(
    sizes,
    forcing_ref, sea_ref, count_ref, state_ref,
    height_ref, resid_ref, tend_ref,
    q_ref, o_ref, side_ref, vert_ref,
    rows_out, rows_in, cols_out, cols_in, corner_out, corner_in, strip_ref, wet_ref,
    basis_ref, diag_ref, part_ref, lon_in, mid_ref, lat_in,
    load_sem, store_sem,
    side_sem, vert_sem, row_sem, col_sem, corner_sem, lon_sem, lat_sem,
):
    n_lon, n_lat, fields, levels, rows = sizes
    planes = fields * levels
    groups = strip_ref.shape[0] // 32
    per_group = 128 // COLS
    ilon, ilat = lax.axis_index("lon"), lax.axis_index("lat")

    def at(dlon, dlat):
        return {
            "lon": lax.rem(ilon + dlon + n_lon, n_lon),
            "lat": lax.rem(ilat + dlat + n_lat, n_lat),
        }

    load = pltpu.make_async_copy(state_ref, q_ref, load_sem)
    load.start()

    barrier = pltpu.get_barrier_semaphore()
    diagonals = [(-1, -1), (1, -1), (-1, 1), (1, 1)]
    for off in range(1, n_lon):
        pl.semaphore_signal(barrier, inc=1, device_id=at(off, 0), device_id_type=MESH)
    for off in range(1, n_lat):
        pl.semaphore_signal(barrier, inc=1, device_id=at(0, off), device_id_type=MESH)
    for dlon, dlat in diagonals:
        pl.semaphore_signal(barrier, inc=1, device_id=at(dlon, dlat), device_id_type=MESH)
    pl.semaphore_wait(barrier, n_lon + n_lat + 2)

    def send(src, dst, sems, index, where):
        copy = pltpu.make_async_remote_copy(
            src_ref=src, dst_ref=dst, send_sem=sems.at[0, index], recv_sem=sems.at[1, index],
            device_id=where, device_id_type=MESH,
        )
        copy.start()
        return copy

    surface = (forcing_ref, sea_ref, count_ref)
    surface_copies = []
    for side, dlon in ((0, 1), (1, -1)):
        for i, ref in enumerate(surface):
            surface_copies.append(send(ref, side_ref.at[i, side], side_sem, i * 2 + side, at(dlon, 0)))
    for v, dlat in ((0, -1), (1, 1)):
        part = pl.ds(0, 8) if v == 0 else pl.ds(rows - 8, 8)
        for h, dlon in ((0, 1), (1, 0), (2, -1)):
            for i, ref in enumerate(surface):
                surface_copies.append(
                    send(ref.at[part], vert_ref.at[i, v, h], vert_sem, (i * 2 + v) * 3 + h, at(dlon, dlat))
                )

    load.wait()
    for i, j in enumerate((0, 1, rows - 2, rows - 1)):
        rows_out[i] = q_ref[pl.ds(j, planes, stride=rows), :]
    state_copies = [
        send(rows_out.at[pl.ds(2, 2)], rows_in.at[pl.ds(0, 2)], row_sem, 0, at(0, 1)),
        send(rows_out.at[pl.ds(0, 2)], rows_in.at[pl.ds(2, 2)], row_sem, 1, at(0, -1)),
    ]

    lane_r = lax.broadcasted_iota(jnp.int32, (rows, 128), 1)
    for g in range(groups):
        inside = min(per_group, planes - g * per_group)

        def pack(s, acc, g=g):
            plane = q_ref[pl.ds(pl.multiple_of((g * per_group + s) * rows, 8), rows), :]
            moved = pltpu.roll(plane, lax.rem(COLS * s + 2, 128), 1)
            return jnp.where(lane_r // COLS == s, moved, acc)

        cols_out[pl.ds(g * rows, rows), :] = lax.fori_loop(
            0, inside, pack, jnp.zeros((rows, 128), jnp.float32), unroll=4
        )
    for i, j in enumerate((0, rows - 1)):
        for g in range(groups):
            corner_out[i, pl.ds(g, 1), :] = cols_out[pl.ds(g * rows + j, 1), :]
    state_copies += [
        send(cols_out, cols_in.at[0], col_sem, 0, at(1, 0)),
        send(cols_out, cols_in.at[1], col_sem, 1, at(-1, 0)),
    ]
    for v, dlat in ((0, -1), (1, 1)):
        for h, dlon in ((0, 1), (1, -1)):
            state_copies.append(
                send(corner_out.at[v], corner_in.at[v, h], corner_sem, v * 2 + h, at(dlon, dlat))
            )

    for copy in surface_copies:
        copy.wait()
    lane8 = lax.broadcasted_iota(jnp.int32, (8, 128), 1)
    above = jnp.where(ilat < n_lat - 1, 1.0, 0.0).astype(jnp.float32)
    below = jnp.where(ilat > 0, 1.0, 0.0).astype(jnp.float32)

    def torus(i):
        ref = surface[i]
        a = jnp.concatenate([ref[...], vert_ref[i, 0, 1], vert_ref[i, 1, 1]], axis=0)
        b = jnp.concatenate(
            [
                jnp.where(lane_r < 64, side_ref[i, 1], side_ref[i, 0]),
                jnp.where(lane8 < 64, vert_ref[i, 0, 2], vert_ref[i, 0, 0]),
                jnp.where(lane8 < 64, vert_ref[i, 1, 2], vert_ref[i, 1, 0]),
            ],
            axis=0,
        )
        return a, b

    row_t = lax.broadcasted_iota(jnp.int32, (rows + 16, 128), 0)
    lane_t = lax.broadcasted_iota(jnp.int32, (rows + 16, 128), 1)
    valid = jnp.where(row_t < rows, 1.0, jnp.where(row_t < rows + 8, above, below))

    force_a, force_b = torus(0)
    sea_a, sea_b = (x * valid for x in torus(1))
    count_a, count_b = torus(2)
    wet_a, wet_b = sea_a * count_a, sea_b * count_b
    sub8 = lax.broadcasted_iota(jnp.int32, (8, 128), 0)
    for i, wet in enumerate((wet_a, wet_b)):
        wet_ref[i, pl.ds(0, rows), :] = wet[:rows]
        wet_ref[i, pl.ds(rows, 8), :] = jnp.where(sub8 < 4, wet[rows : rows + 8], wet[rows + 8 :])
    depth_a, depth_b = wet_a / levels, wet_b / levels
    da, db = east(depth_a, depth_b, lane_t)
    ea, eb = jnp.minimum(depth_a, da), jnp.minimum(depth_b, db)
    wa, wb = west(ea, eb, lane_t)
    na, nb = jnp.minimum(depth_a, north(depth_a)), jnp.minimum(depth_b, north(depth_b))
    sa, sb = south(na), south(nb)
    diag_a = DAMPING + ea + wa + na + sa
    diag_b = DAMPING + eb + wb + nb + sb
    inv_a, inv_b = 1.0 / diag_a, 1.0 / diag_b
    va, vb = sea_a * force_a * inv_a, sea_b * force_b * inv_b
    ea, wa, na, sa = (c * inv_a for c in (ea, wa, na, sa))
    eb, wb, nb, sb = (c * inv_b for c in (eb, wb, nb, sb))
    diag = diag_a[:rows]
    diag_ref[...] = diag
    basis = [va[:rows]]
    for _ in range(ITERS):
        qe, qeb = east(va, vb, lane_t)
        qw, qwb = west(va, vb, lane_t)
        va, vb = (
            ea * qe + wa * qw + na * north(va) + sa * south(va),
            eb * qeb + wb * qwb + nb * north(vb) + sb * south(vb),
        )
        basis.append(va[:rows])
    for i, v in enumerate(basis):
        basis_ref[i] = v
    moments = []
    for m in range(2 * ITERS):
        moments.append(jnp.sum(diag * basis[m // 2] * basis[(m + 1) // 2], axis=0, keepdims=True))
    part_ref[...] = jnp.concatenate(moments, axis=0)
    lon_copies = [
        send(part_ref, lon_in.at[off - 1], lon_sem, off - 1, at(off, 0)) for off in range(1, n_lon)
    ]

    for copy in state_copies:
        copy.wait()
    left_slot = lane_r % COLS < 2
    left8 = lane8 % COLS < 2
    for g in range(groups):
        span = pl.ds(g * rows, rows)
        strip_ref[pl.ds(g * 32, rows), :] = jnp.where(left_slot, cols_in[0, span, :], cols_in[1, span, :])
        one = pl.ds(g, 1)
        up = jnp.where(left8[:1], corner_in[0, 0, one, :], corner_in[0, 1, one, :])
        down = jnp.where(left8[:1], corner_in[1, 0, one, :], corner_in[1, 1, one, :])
        strip_ref[pl.ds(g * 32 + rows, 8), :] = jnp.where(sub8 < 4, up, down)

    tall = rows + 8
    lane = lax.broadcasted_iota(jnp.int32, (tall, 128), 1)

    def plane_of(n):
        body = q_ref[pl.ds(pl.multiple_of(n * rows, 8), rows), :]
        one = pl.ds(n, 1)
        rim = jnp.where(
            sub8 < 4,
            jnp.where(sub8 == 0, rows_in[2, one, :], rows_in[3, one, :]),
            jnp.where(sub8 == 6, rows_in[0, one, :], rows_in[1, one, :]),
        )
        a = jnp.concatenate([body, rim], axis=0)
        strip = strip_ref[pl.ds(pl.multiple_of(n // per_group * 32, 8), tall), :]
        b = pltpu.roll(strip, lax.rem(128 - (COLS * (n % per_group) + 2) + 128, 128), 1)
        return a, b

    def level(k, carry):
        kf = k.astype(jnp.float32)
        aa = jnp.where(kf < wet_ref[0], 1.0, 0.0)
        ab = jnp.where(kf < wet_ref[1], 1.0, 0.0)
        ae, be = east(aa, ab, lane)
        ae, be = aa * ae, ab * be
        an, bn = aa * north(aa), ab * north(ab)
        ua, ub = plane_of(2 * levels + k)
        ue, ueb = east(ua, ub, lane)
        ue, ueb = 0.25 * ae * (ua + ue), 0.25 * be * (ub + ueb)
        va, _ = plane_of(3 * levels + k)
        vn = 0.25 * an * (va + north(va))
        for f in range(fields):
            n = f * levels + k
            qa, qb = plane_of(n)
            qe, qeb = east(qa, qb, lane)
            qn, qnb = north(qa), north(qb)
            fx, fxb = ae * (qe - qa), be * (qeb - qb)
            fw, fwb = west(fx, fxb, lane)
            fy, fyb = an * (qn - qa), bn * (qnb - qb)
            la, lb = fx - fw + fy - south(fy), fxb - fwb + fyb - south(fyb)
            le, leb = east(la, lb, lane)
            gx = ue * (qa + qe) + VISCOSITY * ae * (le - la)
            gxb = ueb * (qb + qeb) + VISCOSITY * be * (leb - lb)
            gy = vn * (qa + qn) + VISCOSITY * an * (north(la) - la)
            gw, _ = west(gx, gxb, lane)
            total = aa * (gw - gx + south(gy) - gy)
            o_ref[pl.ds(pl.multiple_of(n * rows, 8), rows), :] = total[:rows]
        return carry

    half = levels // 2
    lax.fori_loop(0, half, level, 0)

    for copy in lon_copies:
        copy.wait()
    mid = part_ref[...]
    for i in range(n_lon - 1):
        mid = mid + lon_in[i]
    mid_ref[...] = mid
    lat_copies = [
        send(mid_ref, lat_in.at[off - 1], lat_sem, off - 1, at(0, off)) for off in range(1, n_lat)
    ]

    lax.fori_loop(half, levels, level, 0)

    store = pltpu.make_async_copy(o_ref, tend_ref, store_sem)
    store.start()

    for copy in lat_copies:
        copy.wait()
    total = mid_ref[...]
    for i in range(n_lat - 1):
        total = total + lat_in[i]
    total = jnp.broadcast_to(jnp.sum(total, axis=1, keepdims=True), (8, 128))
    mu = [total[m : m + 1] for m in range(2 * ITERS)]

    def inner(x, y):
        sums = [None] * (len(x) + len(y) - 1)
        for i, xi in enumerate(x):
            for j, yj in enumerate(y):
                sums[i + j] = xi * yj if sums[i + j] is None else sums[i + j] + xi * yj
        out = sums[0] * mu[0]
        for m in range(1, len(sums)):
            out = out + sums[m] * mu[m]
        return out

    one = jnp.ones((1, 128), jnp.float32)
    zero = jnp.zeros((1, 128), jnp.float32)
    z, p, h = [one], [one], []
    rz = mu[0]
    for it in range(ITERS):
        image = [hi - lo for hi, lo in zip(p + [zero], [zero] + p)]
        alpha = rz / inner(p, image)
        h = [x + alpha * y for x, y in zip(h + [zero], p)]
        z = [x - alpha * y for x, y in zip(z + [zero], image)]
        if it + 1 < ITERS:
            new = inner(z, z)
            beta = new / rz
            p = [x + beta * y for x, y in zip(z, p + [zero])]
            rz = new
    height = h[0] * basis_ref[0]
    for i in range(1, ITERS):
        height = height + h[i] * basis_ref[i]
    resid = z[0] * basis_ref[0]
    for i in range(1, ITERS + 1):
        resid = resid + z[i] * basis_ref[i]
    height_ref[...] = height
    resid_ref[...] = diag_ref[...] * resid
    store.wait()


def per_device(n_lon, n_lat, forcing, sea, count, state):
    fields, levels, rows, width = state.shape
    planes = fields * levels
    per_group = 128 // COLS
    groups = -(-planes // per_group)
    corner_rows = -(-groups // 8) * 8
    sizes = (n_lon, n_lat, fields, levels, rows)
    f32 = jnp.float32
    vmem = pl.BlockSpec(memory_space=pltpu.VMEM)
    hbm = pl.BlockSpec(memory_space=pl.ANY)
    dma = pltpu.SemaphoreType.DMA
    height, resid, tend = pl.pallas_call(
        functools.partial(kernel, sizes),
        out_shape=(
            jax.ShapeDtypeStruct((rows, width), f32),
            jax.ShapeDtypeStruct((rows, width), f32),
            jax.ShapeDtypeStruct((planes * rows, width), f32),
        ),
        in_specs=[vmem, vmem, vmem, hbm],
        out_specs=(vmem, vmem, hbm),
        scratch_shapes=[
            pltpu.VMEM((planes * rows, width), f32),
            pltpu.VMEM((planes * rows, width), f32),
            pltpu.VMEM((3, 2, rows, width), f32),
            pltpu.VMEM((3, 2, 3, 8, width), f32),
            pltpu.VMEM((4, planes, width), f32),
            pltpu.VMEM((4, planes, width), f32),
            pltpu.VMEM((groups * rows, width), f32),
            pltpu.VMEM((2, groups * rows, width), f32),
            pltpu.VMEM((2, corner_rows, width), f32),
            pltpu.VMEM((2, 2, corner_rows, width), f32),
            pltpu.VMEM((groups * 32, width), f32),
            pltpu.VMEM((2, rows + 8, width), f32),
            pltpu.VMEM((ITERS + 1, rows, width), f32),
            pltpu.VMEM((rows, width), f32),
            pltpu.VMEM((8, width), f32),
            pltpu.VMEM((n_lon - 1, 8, width), f32),
            pltpu.VMEM((8, width), f32),
            pltpu.VMEM((n_lat - 1, 8, width), f32),
            dma,
            dma,
            dma((2, 6)),
            dma((2, 18)),
            dma((2, 2)),
            dma((2, 2)),
            dma((2, 4)),
            dma((2, n_lon - 1)),
            dma((2, n_lat - 1)),
        ],
        compiler_params=pltpu.CompilerParams(collective_id=0, has_side_effects=True),
    )(forcing, sea.astype(f32), count.astype(f32), state.reshape(planes * rows, width))
    return height, resid, tend.reshape(state.shape)


def solution(mesh):
    return jax.shard_map(
        functools.partial(per_device, mesh.shape["lon"], mesh.shape["lat"]),
        mesh=mesh,
        in_specs=(P("lat", "lon"), P("lat", "lon"), P("lat", "lon"), P(None, None, "lat", "lon")),
        out_specs=(P("lat", "lon"), P("lat", "lon"), P(None, None, "lat", "lon")),
        check_vma=False,
    )
```

```python
import functools

import jax
import jax.numpy as jnp
from jax import lax
from jax.experimental import pallas as pl
from jax.experimental.pallas import tpu as pltpu
from jax.sharding import PartitionSpec as P

ITERS = 4
DAMPING = 0.05
VISCOSITY = 0.02
STEP = 8
COLS = 4
MESH = pl.DeviceIdType.MESH


def east(a, b, lane):
    ra, rb = pltpu.roll(a, 127, 1), pltpu.roll(b, 127, 1)
    keep = lane < 127
    return jnp.where(keep, ra, rb), jnp.where(keep, rb, ra)


def west(a, b, lane):
    ra, rb = pltpu.roll(a, 1, 1), pltpu.roll(b, 1, 1)
    keep = lane > 0
    return jnp.where(keep, ra, rb), jnp.where(keep, rb, ra)


def north(x):
    return pltpu.roll(x, x.shape[0] - 1, 0)


def south(x):
    return pltpu.roll(x, 1, 0)


def kernel(
    sizes,
    forcing_ref, sea_ref, count_ref, state_ref,
    height_ref, resid_ref, tend_ref,
    q_ref, o_ref, side_ref, sidei_ref, vert_ref, verti_ref,
    rows_out, rows_in, cols_out, cols_in, corner_out, corner_in, strip_ref, slap_ref,
    face_ref, edge_ref, basis_ref, diag_ref, part_ref, lon_in, mid_ref, lat_in,
    load_sem, store_sem,
    side_sem, vert_sem, row_sem, col_sem, corner_sem, lon_sem, lat_sem,
):
    n_lon, n_lat, fields, levels, rows = sizes
    chunks = levels // STEP
    per_chunk = fields * STEP
    tall = rows + 8
    ilon, ilat = lax.axis_index("lon"), lax.axis_index("lat")
    has = {1: ilat < n_lat - 1, -1: ilat > 0}

    def at(dlon, dlat):
        return {
            "lon": lax.rem(ilon + dlon + n_lon, n_lon),
            "lat": lax.rem(ilat + dlat + n_lat, n_lat),
        }

    barrier = pltpu.get_barrier_semaphore()
    for off in range(1, n_lon):
        pl.semaphore_signal(barrier, inc=1, device_id=at(off, 0), device_id_type=MESH)
    for off in range(1, n_lat):
        pl.semaphore_signal(barrier, inc=1, device_id=at(0, off), device_id_type=MESH)
    for dlon, dlat in ((-1, -1), (1, -1), (-1, 1), (1, 1)):
        pl.semaphore_signal(barrier, inc=1, device_id=at(dlon, dlat), device_id_type=MESH)

    def span(c, f):
        return pl.ds((f * levels + c * STEP) * rows, STEP * rows)

    loads = []
    for c in range(chunks):
        loads.append([])
        for f in range(fields):
            load = pltpu.make_async_copy(
                state_ref.at[span(c, f)], q_ref.at[span(c, f)], load_sem.at[c, f]
            )
            load.start()
            loads[c].append(load)

    def remote(src, dst, sems, index, where):
        return pltpu.make_async_remote_copy(
            src_ref=src, dst_ref=dst, send_sem=sems.at[(0,) + index], recv_sem=sems.at[(1,) + index],
            device_id=where, device_id_type=MESH,
        )

    def send(*args):
        copy = remote(*args)
        copy.start()
        return copy

    def send_lat(copies, dlat):
        @pl.when(has[dlat])
        def _():
            for copy in copies:
                copy.start()

    def wait_lat(copies, dlat):
        @pl.when(has[dlat])
        def _():
            for copy in copies:
                copy.wait_send()

        @pl.when(has[-dlat])
        def _():
            for copy in copies:
                copy.wait_recv()

    for v, dlat in ((0, 1), (1, -1)):
        @pl.when(jnp.logical_not(has[dlat]))
        def _(v=v):
            vert_ref[v] = jnp.zeros_like(vert_ref[v])
            verti_ref[v] = jnp.zeros_like(verti_ref[v])
            corner_in[v] = jnp.zeros_like(corner_in[v])
            for c in range(chunks):
                rows_in[c, pl.ds(2 - 2 * v, 2)] = jnp.zeros_like(rows_in[c, pl.ds(2 - 2 * v, 2)])

    lane_r = lax.broadcasted_iota(jnp.int32, (rows, 128), 1)
    sub8 = lax.broadcasted_iota(jnp.int32, (8, 128), 0)
    lane8 = lax.broadcasted_iota(jnp.int32, (8, 128), 1)

    def pack(c):
        for load in loads[c]:
            load.wait()
        for i, j in enumerate((0, 1, rows - 2, rows - 1)):
            for f in range(fields):
                rows_out[c, i, pl.ds(f * STEP, STEP), :] = q_ref[
                    pl.ds((f * levels + c * STEP) * rows + j, STEP, stride=rows), :
                ]
        packed = jnp.zeros((rows, 128), jnp.float32)
        for f in range(fields):
            for kk in range(STEP):
                s = f * STEP + kk
                plane = q_ref[pl.ds((f * levels + c * STEP + kk) * rows, rows), :]
                moved = pltpu.roll(plane, (COLS * s + 2) % 128, 1)
                packed = jnp.where(lane_r // COLS == s, moved, packed)
        cols_out[c] = packed
        corner_out[c] = jnp.where(sub8 < 4, packed[:8], packed[rows - 8 :])

    pack(0)
    pl.semaphore_wait(barrier, n_lon + n_lat + 2)

    surface = ((forcing_ref, side_ref, vert_ref), (sea_ref, sidei_ref, verti_ref), (count_ref, sidei_ref, verti_ref))
    slot = (0, 0, 1)
    lon_blocks = []
    for i, (ref, side_in, _) in enumerate(surface):
        for side, dlon in ((0, 1), (1, -1)):
            lon_blocks.append(send(ref, side_in.at[slot[i], side], side_sem, (i, side), at(dlon, 0)))
    lat_blocks = []
    for v, dlat in ((0, -1), (1, 1)):
        part = pl.ds(0, 8) if v == 0 else pl.ds(rows - 8, 8)
        lat_blocks.append([
            remote(ref.at[part], vert_in.at[v, slot[i], h], vert_sem, (v, i, h), at(dlon, dlat))
            for i, (ref, _, vert_in) in enumerate(surface)
            for h, dlon in ((0, 1), (1, 0), (2, -1))
        ])
        send_lat(lat_blocks[v], dlat)

    col_copies, row_copies = [], []
    for c in range(chunks):
        if c > 0:
            pack(c)
        col_copies.append([
            send(cols_out.at[c], cols_in.at[c, h], col_sem, (c, h), at(dlon, 0))
            for h, dlon in ((0, 1), (1, -1))
        ])
        row_copies.append([])
        for v, dlat in ((0, -1), (1, 1)):
            row_copies[c].append(
                [remote(rows_out.at[c, pl.ds(2 * v, 2)], rows_in.at[c, pl.ds(2 - 2 * v, 2)],
                        row_sem, (c, v), at(0, dlat))]
                + [
                    remote(corner_out.at[c], corner_in.at[v, c, h], corner_sem, (c, v, h), at(dlon, dlat))
                    for h, dlon in ((0, 1), (1, -1))
                ]
            )
            send_lat(row_copies[c][v], dlat)

    for copy in lon_blocks:
        copy.wait()
    wait_lat(lat_blocks[0], -1)
    wait_lat(lat_blocks[1], 1)

    def torus(i):
        ref, side_in, vert_in = surface[i]
        j = slot[i]
        a = jnp.concatenate([ref[...], vert_in[0, j, 1], vert_in[1, j, 1]], axis=0)
        b = jnp.concatenate(
            [
                jnp.where(lane_r < 64, side_in[j, 1], side_in[j, 0]),
                jnp.where(lane8 < 64, vert_in[0, j, 2], vert_in[0, j, 0]),
                jnp.where(lane8 < 64, vert_in[1, j, 2], vert_in[1, j, 0]),
            ],
            axis=0,
        )
        return a.astype(jnp.float32), b.astype(jnp.float32)

    lane_t = lax.broadcasted_iota(jnp.int32, (rows + 16, 128), 1)
    force_a, force_b = torus(0)
    sea_a, sea_b = torus(1)
    count_a, count_b = torus(2)
    wet_a, wet_b = sea_a * count_a, sea_b * count_b
    depth_a, depth_b = wet_a / levels, wet_b / levels
    da, db = east(depth_a, depth_b, lane_t)
    ea, eb = jnp.minimum(depth_a, da), jnp.minimum(depth_b, db)
    wa, wb = west(ea, eb, lane_t)
    na, nb = jnp.minimum(depth_a, north(depth_a)), jnp.minimum(depth_b, north(depth_b))
    sa, sb = south(na), south(nb)
    diag_a = DAMPING + ea + wa + na + sa
    diag_b = DAMPING + eb + wb + nb + sb
    inv_a, inv_b = 1.0 / diag_a, 1.0 / diag_b
    va, vb = sea_a * force_a * inv_a, sea_b * force_b * inv_b
    ea, wa, na, sa = (c * inv_a for c in (ea, wa, na, sa))
    eb, wb, nb, sb = (c * inv_b for c in (eb, wb, nb, sb))
    diag = diag_a[:rows]
    diag_ref[...] = diag
    basis = [va[:rows]]
    for _ in range(ITERS):
        qe, qeb = east(va, vb, lane_t)
        qw, qwb = west(va, vb, lane_t)
        va, vb = (
            ea * qe + wa * qw + na * north(va) + sa * south(va),
            eb * qeb + wb * qwb + nb * north(vb) + sb * south(vb),
        )
        basis.append(va[:rows])
    for i, v in enumerate(basis):
        basis_ref[i] = v
    moments = []
    for m in range(2 * ITERS):
        moments.append(jnp.sum(diag * basis[m // 2] * basis[(m + 1) // 2], axis=0, keepdims=True))
    part_ref[...] = jnp.concatenate(moments, axis=0)
    lon_copies = [
        send(part_ref, lon_in.at[off - 1], lon_sem, (off - 1,), at(off, 0)) for off in range(1, n_lon)
    ]

    def squeeze(x):
        return jnp.concatenate([x[:rows], jnp.where(sub8 < 4, x[rows : rows + 8], x[rows + 8 :])], axis=0)

    wet_a, wet_b = squeeze(wet_a), squeeze(wet_b)
    lane = lax.broadcasted_iota(jnp.int32, (tall, 128), 1)
    wet_e, _ = east(wet_a, wet_b, lane)
    wet_w, _ = west(wet_a, wet_b, lane)
    for i, other in enumerate((wet_a, wet_e, wet_w, north(wet_a), south(wet_a))):
        face_ref[i] = jnp.minimum(wet_a, other)
    def spread(first, second):
        shape = (tall, 128)
        return jnp.where(lane % COLS < 2, jnp.broadcast_to(first, shape), jnp.broadcast_to(second, shape))

    wet_c = spread(wet_b[:, 0:1], wet_b[:, 127:128])
    wet_o = spread(wet_b[:, 1:2], wet_b[:, 126:127])
    wet_i = spread(wet_a[:, 127:128], wet_a[:, 0:1])
    for i, other in enumerate((wet_i, wet_o, north(wet_c), south(wet_c))):
        edge_ref[i] = jnp.minimum(wet_c, other)[:rows]

    near_r = lane_r % COLS < 2
    near = lane % COLS < 2

    def strips(c):
        for copy in col_copies[c]:
            copy.wait()
        wait_lat(row_copies[c][0], -1)
        wait_lat(row_copies[c][1], 1)
        outer = jnp.concatenate(
            [
                jnp.where(near_r, cols_in[c, 0], cols_in[c, 1]),
                jnp.where(
                    sub8 < 4,
                    jnp.where(lane8 % COLS < 2, corner_in[0, c, 0], corner_in[0, c, 1]),
                    jnp.where(lane8 % COLS < 2, corner_in[1, c, 0], corner_in[1, c, 1]),
                ),
            ],
            axis=0,
        )
        center = jnp.where(near, pltpu.roll(outer, 127, 1), pltpu.roll(outer, 1, 1))
        outer = jnp.where(near, pltpu.roll(outer, 126, 1), pltpu.roll(outer, 2, 1))[:rows]
        strip_ref[c] = center
        mid = center[:rows]
        kf = (c * STEP + (lane_r // COLS) % STEP).astype(jnp.float32)
        others = (cols_out[c], outer, north(center)[:rows], south(center)[:rows])
        total = jnp.zeros_like(mid)
        for i, other in enumerate(others):
            total = total + jnp.where(kf < edge_ref[i], other - mid, 0.0)
        slap_ref[c] = total

    def chunk(c):
        strips(c)

        def level(kk, carry):
            kf = (c * STEP + kk).astype(jnp.float32)
            here = kf < face_ref[0, pl.ds(0, rows), :]
            oe, ow, on, os = (kf < face_ref[i] for i in range(1, 5))
            oe_r, ow_r = oe[:rows], ow[:rows]

            def plane(f):
                s = f * STEP + kk
                base = pl.multiple_of((f * levels + c * STEP + kk) * rows, 8)
                one = pl.ds(s, 1)
                rim = jnp.where(
                    sub8 < 4,
                    jnp.where(sub8 == 0, rows_in[c, 2, one, :], rows_in[c, 3, one, :]),
                    jnp.where(sub8 == 6, rows_in[c, 0, one, :], rows_in[c, 1, one, :]),
                )
                q = jnp.concatenate([q_ref[pl.ds(base, rows), :], rim], axis=0)
                shift = lax.rem(254 - COLS * s, 128)
                edge = pltpu.roll(strip_ref[c], shift, 1)
                qe = jnp.where(lane < 127, pltpu.roll(q, 127, 1), edge)
                qw = jnp.where(lane > 0, pltpu.roll(q, 1, 1), edge)
                return base, shift, q, qe, qw, north(q), south(q)

            planes = {}
            planes[2] = plane(2)
            _, _, u, u_e, u_w, _, _ = planes[2]
            ue = jnp.where(oe_r, 0.25 * (u + u_e)[:rows], 0.0)
            uw = jnp.where(ow_r, 0.25 * (u + u_w)[:rows], 0.0)
            planes[3] = plane(3)
            _, _, v, _, _, v_n, v_s = planes[3]
            vn = jnp.where(on[:rows], 0.25 * (v + v_n)[:rows], 0.0)
            vs = jnp.where(os[:rows], 0.25 * (v + v_s)[:rows], 0.0)
            for f in (2, 3, 0, 1):
                base, shift, q, qe, qw, qn, qs = planes[f] if f in planes else plane(f)
                lap = (
                    jnp.where(oe, qe - q, 0.0) + jnp.where(ow, qw - q, 0.0)
                ) + (jnp.where(on, qn - q, 0.0) + jnp.where(os, qs - q, 0.0))
                near_lap = pltpu.roll(slap_ref[c], shift, 1)
                mid = lap[:rows]
                le = jnp.where(lane_r < 127, pltpu.roll(mid, 127, 1), near_lap)
                lw = jnp.where(lane_r > 0, pltpu.roll(mid, 1, 1), near_lap)
                ln, ls = north(lap)[:rows], south(lap)[:rows]
                again = (
                    jnp.where(oe_r, le - mid, 0.0) + jnp.where(ow_r, lw - mid, 0.0)
                ) + (jnp.where(on[:rows], ln - mid, 0.0) + jnp.where(os[:rows], ls - mid, 0.0))
                qm = q[:rows]
                flux = (ue * (qm + qe[:rows]) - uw * (qm + qw[:rows])) + (
                    vn * (qm + qn[:rows]) - vs * (qm + qs[:rows])
                )
                o_ref[pl.ds(base, rows), :] = jnp.where(here, -flux - VISCOSITY * again, 0.0)
            return carry

        lax.fori_loop(0, STEP, level, 0)
        stores = []
        for f in range(fields):
            store = pltpu.make_async_copy(
                o_ref.at[span(c, f)], tend_ref.at[span(c, f)], store_sem.at[c, f]
            )
            store.start()
            stores.append(store)
        return stores

    turn = min(2, chunks)
    stores = []
    for c in range(turn):
        stores += chunk(c)

    for copy in lon_copies:
        copy.wait()
    total = part_ref[...]
    for i in range(n_lon - 1):
        total = total + lon_in[i]
    mid_ref[...] = total
    lat_copies = [
        send(mid_ref, lat_in.at[off - 1], lat_sem, (off - 1,), at(0, off)) for off in range(1, n_lat)
    ]

    for c in range(turn, chunks):
        stores += chunk(c)

    for copy in lat_copies:
        copy.wait()
    total = mid_ref[...]
    for i in range(n_lat - 1):
        total = total + lat_in[i]
    total = jnp.broadcast_to(jnp.sum(total, axis=1, keepdims=True), (8, 128))
    mu = [total[m : m + 1] for m in range(2 * ITERS)]

    def inner(x, y):
        sums = [None] * (len(x) + len(y) - 1)
        for i, xi in enumerate(x):
            for j, yj in enumerate(y):
                sums[i + j] = xi * yj if sums[i + j] is None else sums[i + j] + xi * yj
        out = sums[0] * mu[0]
        for m in range(1, len(sums)):
            out = out + sums[m] * mu[m]
        return out

    one = jnp.ones((1, 128), jnp.float32)
    zero = jnp.zeros((1, 128), jnp.float32)
    z, p, h = [one], [one], []
    rz = mu[0]
    for it in range(ITERS):
        image = [hi - lo for hi, lo in zip(p + [zero], [zero] + p)]
        alpha = rz / inner(p, image)
        h = [x + alpha * y for x, y in zip(h + [zero], p)]
        z = [x - alpha * y for x, y in zip(z + [zero], image)]
        if it + 1 < ITERS:
            new = inner(z, z)
            beta = new / rz
            p = [x + beta * y for x, y in zip(z, p + [zero])]
            rz = new
    height = h[0] * basis_ref[0]
    for i in range(1, ITERS):
        height = height + h[i] * basis_ref[i]
    resid = z[0] * basis_ref[0]
    for i in range(1, ITERS + 1):
        resid = resid + z[i] * basis_ref[i]
    height_ref[...] = height
    resid_ref[...] = diag_ref[...] * resid
    for store in stores:
        store.wait()


def per_device(n_lon, n_lat, forcing, sea, count, state):
    fields, levels, rows, width = state.shape
    planes = fields * levels
    chunks = levels // STEP
    per_chunk = fields * STEP
    assert levels % STEP == 0 and per_chunk * COLS == width == 128 and rows % 8 == 0 and rows >= 16
    sizes = (n_lon, n_lat, fields, levels, rows)
    f32 = jnp.float32
    vmem = pl.BlockSpec(memory_space=pltpu.VMEM)
    hbm = pl.BlockSpec(memory_space=pl.ANY)
    dma = pltpu.SemaphoreType.DMA
    height, resid, tend = pl.pallas_call(
        functools.partial(kernel, sizes),
        out_shape=(
            jax.ShapeDtypeStruct((rows, width), f32),
            jax.ShapeDtypeStruct((rows, width), f32),
            jax.ShapeDtypeStruct((planes * rows, width), f32),
        ),
        in_specs=[vmem, vmem, vmem, hbm],
        out_specs=(vmem, vmem, hbm),
        scratch_shapes=[
            pltpu.VMEM((planes * rows, width), f32),
            pltpu.VMEM((planes * rows, width), f32),
            pltpu.VMEM((1, 2, rows, width), f32),
            pltpu.VMEM((2, 2, rows, width), jnp.int32),
            pltpu.VMEM((2, 1, 3, 8, width), f32),
            pltpu.VMEM((2, 2, 3, 8, width), jnp.int32),
            pltpu.VMEM((chunks, 4, per_chunk, width), f32),
            pltpu.VMEM((chunks, 4, per_chunk, width), f32),
            pltpu.VMEM((chunks, rows, width), f32),
            pltpu.VMEM((chunks, 2, rows, width), f32),
            pltpu.VMEM((chunks, 8, width), f32),
            pltpu.VMEM((2, chunks, 2, 8, width), f32),
            pltpu.VMEM((chunks, rows + 8, width), f32),
            pltpu.VMEM((chunks, rows, width), f32),
            pltpu.VMEM((5, rows + 8, width), f32),
            pltpu.VMEM((4, rows, width), f32),
            pltpu.VMEM((ITERS + 1, rows, width), f32),
            pltpu.VMEM((rows, width), f32),
            pltpu.VMEM((8, width), f32),
            pltpu.VMEM((n_lon - 1, 8, width), f32),
            pltpu.VMEM((8, width), f32),
            pltpu.VMEM((n_lat - 1, 8, width), f32),
            dma((chunks, fields)),
            dma((chunks, fields)),
            dma((2, 3, 2)),
            dma((2, 2, 3, 3)),
            dma((2, chunks, 2)),
            dma((2, chunks, 2)),
            dma((2, chunks, 2, 2)),
            dma((2, n_lon - 1)),
            dma((2, n_lat - 1)),
        ],
        compiler_params=pltpu.CompilerParams(collective_id=0, has_side_effects=True),
    )(forcing, sea, count, state.reshape(planes * rows, width))
    return height, resid, tend.reshape(state.shape)


def solution(mesh):
    return jax.shard_map(
        functools.partial(per_device, mesh.shape["lon"], mesh.shape["lat"]),
        mesh=mesh,
        in_specs=(P("lat", "lon"), P("lat", "lon"), P("lat", "lon"), P(None, None, "lat", "lon")),
        out_specs=(P("lat", "lon"), P("lat", "lon"), P(None, None, "lat", "lon")),
        check_vma=False,
    )
```

```python
import functools

import jax
import jax.numpy as jnp
from jax import lax
from jax.experimental import pallas as pl
from jax.experimental.pallas import tpu as pltpu
from jax.sharding import PartitionSpec as P

ITERS = 4
DAMPING = 0.05
VISCOSITY = 0.02
STEP = 8
COLS = 4
MESH = pl.DeviceIdType.MESH


def east(a, b, lane):
    ra, rb = pltpu.roll(a, 127, 1), pltpu.roll(b, 127, 1)
    keep = lane < 127
    return jnp.where(keep, ra, rb), jnp.where(keep, rb, ra)


def west(a, b, lane):
    ra, rb = pltpu.roll(a, 1, 1), pltpu.roll(b, 1, 1)
    keep = lane > 0
    return jnp.where(keep, ra, rb), jnp.where(keep, rb, ra)


def north(x):
    return pltpu.roll(x, x.shape[0] - 1, 0)


def south(x):
    return pltpu.roll(x, 1, 0)


def kernel(
    sizes,
    forcing_ref, sea_ref, count_ref, state_ref,
    height_ref, resid_ref, tend_ref,
    q_ref, o_ref, side_ref, sidei_ref, vert_ref, verti_ref,
    rows_out, rows_in, cols_out, cols_in, corner_out, corner_in, strip_ref, slap_ref,
    face_ref, edge_ref, basis_ref, diag_ref, part_ref, lon_in, mid_ref, lat_in,
    load_sem, store_sem,
    side_sem, vert_sem, row_sem, col_sem, corner_sem, lon_sem, lat_sem,
):
    n_lon, n_lat, fields, levels, rows = sizes
    chunks = levels // STEP
    per_chunk = fields * STEP
    tall = rows + 8
    ilon, ilat = lax.axis_index("lon"), lax.axis_index("lat")
    has = {1: ilat < n_lat - 1, -1: ilat > 0}

    def at(dlon, dlat):
        return {
            "lon": lax.rem(ilon + dlon + n_lon, n_lon),
            "lat": lax.rem(ilat + dlat + n_lat, n_lat),
        }

    barrier = pltpu.get_barrier_semaphore()
    for off in range(1, n_lon):
        pl.semaphore_signal(barrier, inc=1, device_id=at(off, 0), device_id_type=MESH)
    for off in range(1, n_lat):
        pl.semaphore_signal(barrier, inc=1, device_id=at(0, off), device_id_type=MESH)
    for dlon, dlat in ((-1, -1), (1, -1), (-1, 1), (1, 1)):
        pl.semaphore_signal(barrier, inc=1, device_id=at(dlon, dlat), device_id_type=MESH)

    def span(c, f):
        return pl.ds((f * levels + c * STEP) * rows, STEP * rows)

    loads = []
    for c in range(chunks):
        loads.append([])
        for f in range(fields):
            load = pltpu.make_async_copy(
                state_ref.at[span(c, f)], q_ref.at[span(c, f)], load_sem.at[c, f]
            )
            load.start()
            loads[c].append(load)

    def remote(src, dst, sems, index, where):
        return pltpu.make_async_remote_copy(
            src_ref=src, dst_ref=dst, send_sem=sems.at[(0,) + index], recv_sem=sems.at[(1,) + index],
            device_id=where, device_id_type=MESH,
        )

    def send(*args):
        copy = remote(*args)
        copy.start()
        return copy

    def send_lat(copies, dlat):
        @pl.when(has[dlat])
        def _():
            for copy in copies:
                copy.start()

    def wait_lat(copies, dlat):
        @pl.when(has[dlat])
        def _():
            for copy in copies:
                copy.wait_send()

        @pl.when(has[-dlat])
        def _():
            for copy in copies:
                copy.wait_recv()

    for v, dlat in ((0, 1), (1, -1)):
        @pl.when(jnp.logical_not(has[dlat]))
        def _(v=v):
            vert_ref[v] = jnp.zeros_like(vert_ref[v])
            verti_ref[v] = jnp.zeros_like(verti_ref[v])
            corner_in[v] = jnp.zeros_like(corner_in[v])
            for c in range(chunks):
                rows_in[c, pl.ds(2 - 2 * v, 2)] = jnp.zeros_like(rows_in[c, pl.ds(2 - 2 * v, 2)])

    lane_r = lax.broadcasted_iota(jnp.int32, (rows, 128), 1)
    sub8 = lax.broadcasted_iota(jnp.int32, (8, 128), 0)
    lane8 = lax.broadcasted_iota(jnp.int32, (8, 128), 1)

    def pack(c):
        for load in loads[c]:
            load.wait()
        for i, j in enumerate((0, 1, rows - 2, rows - 1)):
            for f in range(fields):
                rows_out[c, i, pl.ds(f * STEP, STEP), :] = q_ref[
                    pl.ds((f * levels + c * STEP) * rows + j, STEP, stride=rows), :
                ]
        packed = jnp.zeros((rows, 128), jnp.float32)
        for f in range(fields):
            for kk in range(STEP):
                s = f * STEP + kk
                plane = q_ref[pl.ds((f * levels + c * STEP + kk) * rows, rows), :]
                moved = pltpu.roll(plane, (COLS * s + 2) % 128, 1)
                packed = jnp.where(lane_r // COLS == s, moved, packed)
        cols_out[c] = packed
        corner_out[c] = jnp.where(sub8 < 4, packed[:8], packed[rows - 8 :])

    pack(0)
    pl.semaphore_wait(barrier, n_lon + n_lat + 2)

    surface = ((forcing_ref, side_ref, vert_ref), (sea_ref, sidei_ref, verti_ref), (count_ref, sidei_ref, verti_ref))
    slot = (0, 0, 1)
    lon_blocks = []
    for i, (ref, side_in, _) in enumerate(surface):
        for side, dlon in ((0, 1), (1, -1)):
            lon_blocks.append(send(ref, side_in.at[slot[i], side], side_sem, (i, side), at(dlon, 0)))
    lat_blocks = []
    for v, dlat in ((0, -1), (1, 1)):
        part = pl.ds(0, 8) if v == 0 else pl.ds(rows - 8, 8)
        lat_blocks.append([
            remote(ref.at[part], vert_in.at[v, slot[i], h], vert_sem, (v, i, h), at(dlon, dlat))
            for i, (ref, _, vert_in) in enumerate(surface)
            for h, dlon in ((0, 1), (1, 0), (2, -1))
        ])
        send_lat(lat_blocks[v], dlat)

    col_copies, row_copies = [], []
    for c in range(chunks):
        if c > 0:
            pack(c)
        col_copies.append([
            send(cols_out.at[c], cols_in.at[c, h], col_sem, (c, h), at(dlon, 0))
            for h, dlon in ((0, 1), (1, -1))
        ])
        row_copies.append([])
        for v, dlat in ((0, -1), (1, 1)):
            row_copies[c].append(
                [remote(rows_out.at[c, pl.ds(2 * v, 2)], rows_in.at[c, pl.ds(2 - 2 * v, 2)],
                        row_sem, (c, v), at(0, dlat))]
                + [
                    remote(corner_out.at[c], corner_in.at[v, c, h], corner_sem, (c, v, h), at(dlon, dlat))
                    for h, dlon in ((0, 1), (1, -1))
                ]
            )
            send_lat(row_copies[c][v], dlat)

    for copy in lon_blocks:
        copy.wait()
    wait_lat(lat_blocks[0], -1)
    wait_lat(lat_blocks[1], 1)

    def torus(i):
        ref, side_in, vert_in = surface[i]
        j = slot[i]
        a = jnp.concatenate([ref[...], vert_in[0, j, 1], vert_in[1, j, 1]], axis=0)
        b = jnp.concatenate(
            [
                jnp.where(lane_r < 64, side_in[j, 1], side_in[j, 0]),
                jnp.where(lane8 < 64, vert_in[0, j, 2], vert_in[0, j, 0]),
                jnp.where(lane8 < 64, vert_in[1, j, 2], vert_in[1, j, 0]),
            ],
            axis=0,
        )
        return a.astype(jnp.float32), b.astype(jnp.float32)

    lane_t = lax.broadcasted_iota(jnp.int32, (rows + 16, 128), 1)
    force_a, force_b = torus(0)
    sea_a, sea_b = torus(1)
    count_a, count_b = torus(2)
    wet_a, wet_b = sea_a * count_a, sea_b * count_b
    depth_a, depth_b = wet_a / levels, wet_b / levels
    da, db = east(depth_a, depth_b, lane_t)
    ea, eb = jnp.minimum(depth_a, da), jnp.minimum(depth_b, db)
    wa, wb = west(ea, eb, lane_t)
    na, nb = jnp.minimum(depth_a, north(depth_a)), jnp.minimum(depth_b, north(depth_b))
    sa, sb = south(na), south(nb)
    diag_a = DAMPING + ea + wa + na + sa
    diag_b = DAMPING + eb + wb + nb + sb
    inv_a, inv_b = 1.0 / diag_a, 1.0 / diag_b
    va, vb = sea_a * force_a * inv_a, sea_b * force_b * inv_b
    ea, wa, na, sa = (c * inv_a for c in (ea, wa, na, sa))
    eb, wb, nb, sb = (c * inv_b for c in (eb, wb, nb, sb))
    diag = diag_a[:rows]
    diag_ref[...] = diag
    basis = [va[:rows]]
    for _ in range(ITERS):
        qe, qeb = east(va, vb, lane_t)
        qw, qwb = west(va, vb, lane_t)
        va, vb = (
            ea * qe + wa * qw + na * north(va) + sa * south(va),
            eb * qeb + wb * qwb + nb * north(vb) + sb * south(vb),
        )
        basis.append(va[:rows])
    for i, v in enumerate(basis):
        basis_ref[i] = v
    moments = []
    for m in range(2 * ITERS):
        moments.append(jnp.sum(diag * basis[m // 2] * basis[(m + 1) // 2], axis=0, keepdims=True))
    part_ref[...] = jnp.concatenate(moments, axis=0)
    lon_copies = [
        send(part_ref, lon_in.at[off - 1], lon_sem, (off - 1,), at(off, 0)) for off in range(1, n_lon)
    ]

    def squeeze(x):
        return jnp.concatenate([x[:rows], jnp.where(sub8 < 4, x[rows : rows + 8], x[rows + 8 :])], axis=0)

    wet_a, wet_b = squeeze(wet_a), squeeze(wet_b)
    lane = lax.broadcasted_iota(jnp.int32, (tall, 128), 1)
    wet_e, _ = east(wet_a, wet_b, lane)
    wet_w, _ = west(wet_a, wet_b, lane)
    for i, other in enumerate((wet_a, wet_e, wet_w, north(wet_a), south(wet_a))):
        face_ref[i] = jnp.minimum(wet_a, other)
    def spread(first, second):
        shape = (tall, 128)
        return jnp.where(lane % COLS < 2, jnp.broadcast_to(first, shape), jnp.broadcast_to(second, shape))

    wet_c = spread(wet_b[:, 0:1], wet_b[:, 127:128])
    wet_o = spread(wet_b[:, 1:2], wet_b[:, 126:127])
    wet_i = spread(wet_a[:, 127:128], wet_a[:, 0:1])
    for i, other in enumerate((wet_i, wet_o, north(wet_c), south(wet_c))):
        edge_ref[i] = jnp.minimum(wet_c, other)[:rows]

    near_r = lane_r % COLS < 2
    near = lane % COLS < 2

    def strips(c):
        for copy in col_copies[c]:
            copy.wait()
        wait_lat(row_copies[c][0], -1)
        wait_lat(row_copies[c][1], 1)
        outer = jnp.concatenate(
            [
                jnp.where(near_r, cols_in[c, 0], cols_in[c, 1]),
                jnp.where(
                    sub8 < 4,
                    jnp.where(lane8 % COLS < 2, corner_in[0, c, 0], corner_in[0, c, 1]),
                    jnp.where(lane8 % COLS < 2, corner_in[1, c, 0], corner_in[1, c, 1]),
                ),
            ],
            axis=0,
        )
        center = jnp.where(near, pltpu.roll(outer, 127, 1), pltpu.roll(outer, 1, 1))
        outer = jnp.where(near, pltpu.roll(outer, 126, 1), pltpu.roll(outer, 2, 1))[:rows]
        strip_ref[c] = center
        mid = center[:rows]
        kf = (c * STEP + (lane_r // COLS) % STEP).astype(jnp.float32)
        others = (cols_out[c], outer, north(center)[:rows], south(center)[:rows])
        total = jnp.zeros_like(mid)
        for i, other in enumerate(others):
            total = total + jnp.where(kf < edge_ref[i], other - mid, 0.0)
        slap_ref[c] = total

    def chunk(c):
        strips(c)

        def level(kk, carry):
            kf = (c * STEP + kk).astype(jnp.float32)
            here = kf < face_ref[0, pl.ds(0, rows), :]
            oe, ow, on, os = (kf < face_ref[i] for i in range(1, 5))
            oe_r, ow_r = oe[:rows], ow[:rows]

            def plane(f):
                s = f * STEP + kk
                base = pl.multiple_of((f * levels + c * STEP + kk) * rows, 8)
                one = pl.ds(s, 1)
                rim = jnp.where(
                    sub8 < 4,
                    jnp.where(sub8 == 0, rows_in[c, 2, one, :], rows_in[c, 3, one, :]),
                    jnp.where(sub8 == 6, rows_in[c, 0, one, :], rows_in[c, 1, one, :]),
                )
                q = jnp.concatenate([q_ref[pl.ds(base, rows), :], rim], axis=0)
                shift = lax.rem(254 - COLS * s, 128)
                edge = pltpu.roll(strip_ref[c], shift, 1)
                qe = jnp.where(lane < 127, pltpu.roll(q, 127, 1), edge)
                qw = jnp.where(lane > 0, pltpu.roll(q, 1, 1), edge)
                return base, shift, q, qe, qw, north(q), south(q)

            planes = {}
            planes[2] = plane(2)
            _, _, u, u_e, u_w, _, _ = planes[2]
            ue = jnp.where(oe_r, 0.25 * (u + u_e)[:rows], 0.0)
            uw = jnp.where(ow_r, 0.25 * (u + u_w)[:rows], 0.0)
            planes[3] = plane(3)
            _, _, v, _, _, v_n, v_s = planes[3]
            vn = jnp.where(on[:rows], 0.25 * (v + v_n)[:rows], 0.0)
            vs = jnp.where(os[:rows], 0.25 * (v + v_s)[:rows], 0.0)
            for f in (2, 3, 0, 1):
                base, shift, q, qe, qw, qn, qs = planes[f] if f in planes else plane(f)
                lap = (
                    jnp.where(oe, qe - q, 0.0) + jnp.where(ow, qw - q, 0.0)
                ) + (jnp.where(on, qn - q, 0.0) + jnp.where(os, qs - q, 0.0))
                near_lap = pltpu.roll(slap_ref[c], shift, 1)
                mid = lap[:rows]
                le = jnp.where(lane_r < 127, pltpu.roll(mid, 127, 1), near_lap)
                lw = jnp.where(lane_r > 0, pltpu.roll(mid, 1, 1), near_lap)
                ln, ls = north(lap)[:rows], south(lap)[:rows]
                again = (
                    jnp.where(oe_r, le - mid, 0.0) + jnp.where(ow_r, lw - mid, 0.0)
                ) + (jnp.where(on[:rows], ln - mid, 0.0) + jnp.where(os[:rows], ls - mid, 0.0))
                qm = q[:rows]
                flux = (ue * (qm + qe[:rows]) - uw * (qm + qw[:rows])) + (
                    vn * (qm + qn[:rows]) - vs * (qm + qs[:rows])
                )
                o_ref[pl.ds(base, rows), :] = jnp.where(here, -flux - VISCOSITY * again, 0.0)
            return carry

        lax.fori_loop(0, STEP, level, 0)
        stores = []
        for f in range(fields):
            store = pltpu.make_async_copy(
                o_ref.at[span(c, f)], tend_ref.at[span(c, f)], store_sem.at[c, f]
            )
            store.start()
            stores.append(store)
        return stores

    turn = min(2, chunks)
    stores = []
    for c in range(turn):
        stores += chunk(c)

    for copy in lon_copies:
        copy.wait()
    total = part_ref[...]
    for i in range(n_lon - 1):
        total = total + lon_in[i]
    mid_ref[...] = total
    lat_copies = [
        send(mid_ref, lat_in.at[off - 1], lat_sem, (off - 1,), at(0, off)) for off in range(1, n_lat)
    ]

    for c in range(turn, chunks):
        stores += chunk(c)

    for copy in lat_copies:
        copy.wait()
    total = mid_ref[...]
    for i in range(n_lat - 1):
        total = total + lat_in[i]
    total = jnp.broadcast_to(jnp.sum(total, axis=1, keepdims=True), (8, 128))
    mu = [total[m : m + 1] for m in range(2 * ITERS)]

    def inner(x, y):
        sums = [None] * (len(x) + len(y) - 1)
        for i, xi in enumerate(x):
            for j, yj in enumerate(y):
                sums[i + j] = xi * yj if sums[i + j] is None else sums[i + j] + xi * yj
        out = sums[0] * mu[0]
        for m in range(1, len(sums)):
            out = out + sums[m] * mu[m]
        return out

    one = jnp.ones((1, 128), jnp.float32)
    zero = jnp.zeros((1, 128), jnp.float32)
    z, p, h = [one], [one], []
    rz = mu[0]
    for it in range(ITERS):
        image = [hi - lo for hi, lo in zip(p + [zero], [zero] + p)]
        alpha = rz / inner(p, image)
        h = [x + alpha * y for x, y in zip(h + [zero], p)]
        z = [x - alpha * y for x, y in zip(z + [zero], image)]
        if it + 1 < ITERS:
            new = inner(z, z)
            beta = new / rz
            p = [x + beta * y for x, y in zip(z, p + [zero])]
            rz = new
    height = h[0] * basis_ref[0]
    for i in range(1, ITERS):
        height = height + h[i] * basis_ref[i]
    resid = z[0] * basis_ref[0]
    for i in range(1, ITERS + 1):
        resid = resid + z[i] * basis_ref[i]
    height_ref[...] = height
    resid_ref[...] = diag_ref[...] * resid
    for store in stores:
        store.wait()


def deliver(height_in, resid_in, tend_in, height_ref, resid_ref, tend_ref, h_buf, r_buf, t_buf, in_sem, out_sem):
    pieces = in_sem.shape[0] - 2
    size = t_buf.shape[0] // pieces
    moves = [(tend_in.at[pl.ds(i * size, size)], t_buf.at[pl.ds(i * size, size)], tend_ref.at[pl.ds(i * size, size)])
             for i in range(pieces)]
    moves += [(height_in, h_buf, height_ref), (resid_in, r_buf, resid_ref)]
    loads = [pltpu.make_async_copy(src, buf, in_sem.at[i]) for i, (src, buf, _) in enumerate(moves)]
    stores = [pltpu.make_async_copy(buf, dst, out_sem.at[i]) for i, (_, buf, dst) in enumerate(moves)]
    for load in loads:
        load.start()
    for load, store in zip(loads, stores):
        load.wait()
        store.start()
    for store in stores:
        store.wait()


def per_device(n_lon, n_lat, forcing, sea, count, state):
    fields, levels, rows, width = state.shape
    planes = fields * levels
    chunks = levels // STEP
    per_chunk = fields * STEP
    assert levels % STEP == 0 and per_chunk * COLS == width == 128 and rows % 8 == 0 and rows >= 16
    sizes = (n_lon, n_lat, fields, levels, rows)
    f32 = jnp.float32
    vmem = pl.BlockSpec(memory_space=pltpu.VMEM)
    hbm = pl.BlockSpec(memory_space=pl.ANY)
    dma = pltpu.SemaphoreType.DMA
    height, resid, tend = pl.pallas_call(
        functools.partial(kernel, sizes),
        out_shape=(
            jax.ShapeDtypeStruct((rows, width), f32),
            jax.ShapeDtypeStruct((rows, width), f32),
            jax.ShapeDtypeStruct((planes * rows, width), f32),
        ),
        in_specs=[vmem, vmem, vmem, hbm],
        out_specs=(vmem, vmem, hbm),
        scratch_shapes=[
            pltpu.VMEM((planes * rows, width), f32),
            pltpu.VMEM((planes * rows, width), f32),
            pltpu.VMEM((1, 2, rows, width), f32),
            pltpu.VMEM((2, 2, rows, width), jnp.int32),
            pltpu.VMEM((2, 1, 3, 8, width), f32),
            pltpu.VMEM((2, 2, 3, 8, width), jnp.int32),
            pltpu.VMEM((chunks, 4, per_chunk, width), f32),
            pltpu.VMEM((chunks, 4, per_chunk, width), f32),
            pltpu.VMEM((chunks, rows, width), f32),
            pltpu.VMEM((chunks, 2, rows, width), f32),
            pltpu.VMEM((chunks, 8, width), f32),
            pltpu.VMEM((2, chunks, 2, 8, width), f32),
            pltpu.VMEM((chunks, rows + 8, width), f32),
            pltpu.VMEM((chunks, rows, width), f32),
            pltpu.VMEM((5, rows + 8, width), f32),
            pltpu.VMEM((4, rows, width), f32),
            pltpu.VMEM((ITERS + 1, rows, width), f32),
            pltpu.VMEM((rows, width), f32),
            pltpu.VMEM((8, width), f32),
            pltpu.VMEM((n_lon - 1, 8, width), f32),
            pltpu.VMEM((8, width), f32),
            pltpu.VMEM((n_lat - 1, 8, width), f32),
            dma((chunks, fields)),
            dma((chunks, fields)),
            dma((2, 3, 2)),
            dma((2, 2, 3, 3)),
            dma((2, chunks, 2)),
            dma((2, chunks, 2)),
            dma((2, chunks, 2, 2)),
            dma((2, n_lon - 1)),
            dma((2, n_lat - 1)),
        ],
        compiler_params=pltpu.CompilerParams(collective_id=0, has_side_effects=True),
    )(forcing, sea, count, state.reshape(planes * rows, width))
    small = jax.ShapeDtypeStruct((rows, width), f32)
    pieces = 2 * fields
    height, resid, tend = pl.pallas_call(
        deliver,
        out_shape=(small, small, jax.ShapeDtypeStruct((planes * rows, width), f32)),
        in_specs=[hbm] * 3,
        out_specs=(hbm,) * 3,
        scratch_shapes=[
            pltpu.VMEM((rows, width), f32),
            pltpu.VMEM((rows, width), f32),
            pltpu.VMEM((planes * rows, width), f32),
            dma((pieces + 2,)),
            dma((pieces + 2,)),
        ],
    )(height, resid, tend)
    return height, resid, tend.reshape(state.shape)


def solution(mesh):
    return jax.shard_map(
        functools.partial(per_device, mesh.shape["lon"], mesh.shape["lat"]),
        mesh=mesh,
        in_specs=(P("lat", "lon"), P("lat", "lon"), P("lat", "lon"), P(None, None, "lat", "lon")),
        out_specs=(P("lat", "lon"), P("lat", "lon"), P(None, None, "lat", "lon")),
        check_vma=False,
    )
```
